32 devices in a mesh: section: 2 (over x), ex: 4 (over z), ey: 4 (over y, core).
Axes of the slice: x: 2, y: 2, z: 4, core: 2. Of those that a mesh axis runs over, the one named last changes fastest.
Arguments:
- section_out: bfloat16 [2, 1024, 7168], P('section', ('ex', 'ey')), may hold values from -6 to 6
- expert_ids: int32 [2, 1024, 2], P('section', ('ex', 'ey')), may hold values from 0 to 3, all different within a row; in each aligned block of 64 rows (0 to 63, 64 to 127, ..., all dimensions but the last counted through in order) at most 48 rows name the same one
- gate_weights: float32 [2, 1024, 2], P('section', ('ex', 'ey')), may hold values from 0.1 to 1
- w_gate_up: bfloat16 [2, 4, 7168, 2, 1024], P('section', 'ey', None, None, 'ex'), may hold values from -0.0625 to 0.0625
- w_down: bfloat16 [2, 4, 1024, 7168], P('section', 'ey', 'ex'), may hold values from -0.1875 to 0.1875
Outputs:
- next_state: bfloat16 [2, 1024, 7168], P('section', ('ex', 'ey'))
The draws below stay inside these ranges and needn't reach their ends.
Inputs may be any that keep to these rules, and one draw needn't show every extreme that they name: `expert_ids`: each row names 2 different experts. In the rows of one device (aligned blocks of 64 rows, all leading dimensions in order) no expert is named by more than 48 rows, and some block of every draw names one expert exactly 48 times.
All inputs are finite; a program needn't handle non-finite values.
Results may differ from the reference program's by a relative error of at most 0.008.
Values may be sent and summed in bfloat16 or wider, within the bound.
A program may use at most 128 MiB of HBM per device.

```python
import math
import jax
import jax.numpy as jnp
import numpy as np
from jax import lax

D = 7168
FF = 1024
TOP = 2
TOK_DEV = 64
SECTIONS = 2
EXPERTS = 4
TOKENS = 1024
CAP = 48
N_EX = 4


def level_of(key, extent, shards, smallest, high):
    loudness, own = 1.0, jax.random.fold_in(key, 6)
    for dim, blocks in shards:
        heights = jnp.exp(jax.random.uniform(jax.random.fold_in(own, dim), (blocks,), jnp.float32, smallest / len(shards), high / len(shards)))
        loudness = loudness * jnp.repeat(heights, extent[dim] // blocks).reshape([-1 if axis == dim else 1 for axis in range(len(extent))])
    return loudness


def shared_out(rng, own, number, rows, number_of, top, reach, slope):
    ranking = jax.random.permutation(rng, number_of)
    crowded, usual = shares(number_of, rows * top, reach, slope, True), shares(number_of, rows * top, reach, slope, False)
    places = jnp.arange(number_of)

    def named(tallies, rotation):
        used = int((tallies > 0).sum())
        fixed = max(1, used // 4)
        shifted = fixed + (places - fixed + rotation * (used - fixed)) % max(1, number_of - fixed)
        return jnp.zeros((number_of,), jnp.int32).at[ranking[jnp.where(places < fixed, places, shifted)]].set(jnp.asarray(tallies, jnp.int32))

    tallies = jnp.where(number % 4 == 0, named(crowded, number // 4), named(usual, number - number // 4 - 1))
    mixed = jax.random.permutation(jax.random.fold_in(own, 3), number_of)
    donor, taker = mixed[0:number_of // 2 * 2:2], mixed[1:number_of // 2 * 2:2]
    room = jnp.minimum(tallies[donor] - 1, reach - tallies[taker]) // 2
    room = jnp.where((donor == ranking[0]) | (taker == ranking[0]) | (tallies[taker] == 0), 0, jnp.maximum(room, 0))
    shifted = jax.random.randint(jax.random.fold_in(own, 4), (number_of // 2,), 0, 1 << 20) % (room + 1)
    tallies = tallies.at[donor].add(-shifted).at[taker].add(shifted)
    items = jnp.searchsorted(jnp.cumsum(tallies), jnp.arange(rows * top), side="right").astype(jnp.int32)
    table = items.reshape(top, rows).T
    table = table[jax.random.permutation(jax.random.fold_in(own, 1), rows)]
    rotation = jax.random.randint(jax.random.fold_in(own, 2), (rows, 1), 0, top)
    return jnp.take_along_axis(table, (jnp.arange(top)[None, :] + rotation) % top, axis=1)


def shares(amount, total, bound, skew, full):
    loads = [(1 << 20) // math.isqrt(standing ** skew) + 1 for standing in range(1, amount + 1)]
    largest = bound if full else min(bound, max(-(-total // amount), total * loads[0] // sum(loads)))
    least = 1 if total - largest >= amount - 1 else 0
    given, spare = [largest] + [least] * (amount - 1), total - largest - least * (amount - 1)
    while spare > 0:
        movable = [i for i in range(1, amount) if given[i] < largest] or [i for i in range(1, amount) if given[i] < bound]
        pool, left = sum([loads[i] for i in movable]), spare
        for i in movable:
            more = min(bound - given[i], max(1, left * loads[i] // pool), spare)
            given[i] = given[i] + more
            spare = spare - more
    return np.array(given)


def centred(key, extent, scale, limit, split=(), held_as=jnp.bfloat16):
    array = scale * jax.random.normal(key, extent, jnp.float32)
    if split:
        array = array * level_of(key, extent, split, -0.22, 0.18)
    return jnp.clip(array, -limit, limit).astype(held_as)


def setup_inputs(seed: int = 0) -> dict:
    key_list = jax.random.split(jax.random.key(seed), 6)
    section_out = centred(key_list[0], (SECTIONS, TOKENS, D), 1.0, 6.0, ((0, 2), (1, 16)))
    expert_ids_keys = jax.random.split(jax.random.fold_in(key_list[1], 1), SECTIONS * TOKENS // TOK_DEV)
    expert_ids_turns = jax.random.permutation(jax.random.fold_in(key_list[1], 3), SECTIONS * TOKENS // TOK_DEV)
    expert_ids = jax.vmap(lambda own, number: shared_out(jax.random.fold_in(key_list[1], 2), own, number, TOK_DEV, EXPERTS, TOP, CAP, 2))(expert_ids_keys, expert_ids_turns).reshape((SECTIONS, TOKENS, TOP))
    gate_weights = jnp.clip(jnp.exp(math.log(1.0) - 2.3025851 * jax.random.uniform(key_list[2], (SECTIONS, TOKENS, TOP), jnp.float32) ** level_of(key_list[2], (SECTIONS, TOKENS, TOP), ((0, 2), (1, 16)), -0.2, 0.2)), 0.1, 1.0)
    w_gate_up = centred(key_list[3], (SECTIONS, EXPERTS, D, 2, FF), D ** -0.5, 0.0625, ((0, 2), (1, 4), (4, 4)))
    w_down = centred(key_list[4], (SECTIONS, EXPERTS, FF, D), FF ** -0.5, 0.1875, ((0, 2), (1, 4), (2, 4)))
    return dict(section_out=section_out, expert_ids=expert_ids, gate_weights=gate_weights, w_gate_up=w_gate_up, w_down=w_down)


def route_section(section_args):
    incoming, chosen_ids, gates, gate_up, down_proj = section_args
    devices = TOKENS // TOK_DEV
    slot_total = devices * CAP
    flat_ids = chosen_ids.reshape(devices, TOK_DEV * TOP)
    one_hot = (flat_ids[:, :, None] == jnp.arange(EXPERTS, dtype=jnp.int32)[None, None, :]).astype(jnp.int32)
    slot_rank = jnp.sum((jnp.cumsum(one_hot, axis=1) - one_hot) * one_hot, axis=2)
    device_ids = jnp.arange(devices, dtype=jnp.int32)[:, None]
    position = (flat_ids * slot_total + device_ids * CAP + slot_rank).reshape(-1).astype(jnp.int32)
    token_of = jnp.arange(TOKENS * TOP, dtype=jnp.int32) // TOP
    source_row = jnp.zeros((EXPERTS * slot_total,), jnp.int32).at[position].set(token_of)
    slice_width = FF // N_EX

    def one_expert(expert_args):
        expert_index, weight_rows, down_rows = expert_args
        chosen_rows = lax.dynamic_slice_in_dim(source_row, expert_index * slot_total, slot_total)
        token_rows = incoming[chosen_rows]
        mixed = jnp.dot(token_rows, weight_rows.reshape(D, 2 * FF), preferred_element_type=jnp.float32)
        hidden = (jax.nn.silu(mixed[:, :FF]) * mixed[:, FF:]).astype(jnp.bfloat16)
        slice_parts = jnp.einsum("rqf,qfd->qrd", hidden.reshape(slot_total, N_EX, slice_width).astype(jnp.float32),
                                 down_rows.reshape(N_EX, slice_width, D).astype(jnp.float32))
        rounded = lax.optimization_barrier(slice_parts.astype(jnp.bfloat16))
        return jnp.sum(rounded.astype(jnp.float32), axis=0).astype(jnp.bfloat16)

    expert_out = lax.map(one_expert, (jnp.arange(EXPERTS, dtype=jnp.int32), gate_up, down_proj))
    picked = expert_out.reshape(EXPERTS * slot_total, D)[position].reshape(TOKENS, TOP, D)
    weighted = jnp.einsum("tkd,tk->td", picked.astype(jnp.float32), gates.astype(jnp.float32))
    return (incoming.astype(jnp.float32) + weighted).astype(jnp.bfloat16)


def reference(section_out, expert_ids, gate_weights, w_gate_up, w_down):
    incoming = jnp.roll(section_out, 1, axis=0)
    return lax.map(route_section, (incoming, expert_ids, gate_weights, w_gate_up, w_down))
```

```python
import functools
import jax
import jax.numpy as jnp
from jax import lax
from jax.experimental import pallas as pl
from jax.experimental.pallas import tpu as pltpu
from jax.sharding import PartitionSpec as P

LANES = 128
VMEM_BYTES = 67043328
MESH = pl.DeviceIdType.MESH
F32, BF16 = jnp.float32, jnp.bfloat16


def spans_of(width, parts):
    tiles = width // LANES
    first = max(1, tiles * 10 // 56)
    cuts = [0, first * LANES]
    for i in range(parts - 1):
        cuts.append((first + (tiles - first) * (i + 1) // (parts - 1)) * LANES)
    return tuple((a, b - a) for a, b in zip(cuts[:-1], cuts[1:]))


def even_spans(width, parts):
    tiles = width // LANES
    cuts = [tiles * i // parts * LANES for i in range(parts + 1)]
    return tuple((a, b - a) for a, b in zip(cuts[:-1], cuts[1:]))


def fused_kernel(S, E, EY, R, D, U, CAPW, ag_spans, y_first, rs_spans, ktile, ntile,
                 x_ref, cw_ref, wgu_ref, wd_ref, out_ref,
                 tok, part, wgu, wd, hid, mix, acc, cw_all, sib_in, y_in, z_in,
                 w_sem, shift_s, ag_r, zs, ys, ss, cw_s, cw_r,
                 rsib_s, rsib_r, ry_s, ry_r, rz_s, rz_r):
    Y = EY // 2
    s, e, yc = lax.axis_index("section"), lax.axis_index("ex"), lax.axis_index("ey")
    y, c = yc // 2, yc % 2
    sib = {"ey": 2 * y + (1 - c)}

    barrier = pltpu.get_barrier_semaphore()
    others = [(i, j) for i in range(E) for j in range(EY) if i or j]
    for i, j in others:
        pl.semaphore_signal(barrier, inc=1, device_id={"ex": (e + i) % E, "ey": (yc + j) % EY}, device_id_type=MESH)
    for d in (1, S - 1):
        pl.semaphore_signal(barrier, inc=1, device_id={"section": (s + d) % S}, device_id_type=MESH)
    loads = [pltpu.make_async_copy(wgu_ref, wgu, w_sem.at[0]), pltpu.make_async_copy(wd_ref, wd, w_sem.at[1])]
    for load in loads:
        load.start()
    pl.semaphore_wait(barrier, len(others) + 2)

    def remote(src, dst, send, recv, device):
        return pltpu.make_async_remote_copy(src_ref=src, dst_ref=dst, send_sem=send, recv_sem=recv,
                                            device_id=device, device_id_type=MESH)

    def rows(core):
        return pl.ds(pl.multiple_of(core * R, R), R)

    def block(ee, cc, h):
        return tok.at[ee, rows(cc), pl.ds(*ag_spans[h])]

    def shift_copy(h):
        return remote(x_ref.at[:, pl.ds(*ag_spans[h])], block(e, yc, h), shift_s.at[h], ag_r.at[e, yc, h],
                      {"section": (s + 1) % S})

    def z_copy(way, ee, yy, h):
        step = 1 - 2 * way
        b = block(ee, 2 * yy + c, h)
        return remote(b, b, zs.at[way, ee, yy, h], ag_r.at[ee, 2 * yy + c, h], {"ex": e + step})

    def y_copy(i, ee, h):
        b = block(ee, yc, h)
        return remote(b, b, ys.at[i, ee, h], ag_r.at[ee, yc, h], {"ey": (yc + 2 * (i + 1)) % EY})

    def sib_copy(ee, yy, h):
        b = block(ee, 2 * yy + c, h)
        return remote(b, b, ss.at[ee, yy, h], ag_r.at[ee, 2 * yy + c, h], sib)

    def arrived(ee, cc, h):
        b = block(ee, cc, h)
        remote(b, b, ss.at[0, 0, 0], ag_r.at[ee, cc, h], sib).wait_recv()

    for h in range(len(ag_spans)):
        shift_copy(h).start()

    def cw_copy(i, j):
        return remote(cw_ref, cw_all.at[e, yc], cw_s.at[i, j], cw_r.at[e, yc],
                      {"ex": (e + i) % E, "ey": (yc + j) % EY})

    for i, j in others:
        cw_copy(i, j).start()
    cw_all[e, yc] = cw_ref[...]

    def spread(ee, yy, h, k, side):
        sib_copy(ee, yy, h).start()
        if side in (None, 0):
            @pl.when(e < E - 1)
            def _():
                z_copy(0, ee, yy, h).start()
        if side in (None, 1):
            @pl.when(e > 0)
            def _():
                z_copy(1, ee, yy, h).start()

    def side_blocks(k):
        if k == 0:
            return [(None, e, None)]
        return [(0, e - k, e >= k), (1, e + k, e + k < E)]

    def guarded(cond, fn):
        if cond is None:
            fn()
        else:
            pl.when(cond)(fn)

    def others_of(y0):
        return [(y0 + 1 + i) % Y for i in range(Y - 1)]

    def z_stage(k):
        for h in range(len(ag_spans)):
            for side, ee, cond in side_blocks(k):
                def go(side=side, ee=ee, h=h):
                    first = h < y_first
                    arrived(ee, yc, h)
                    if not first or k == 0:
                        for i in range(Y - 1):
                            y_copy(i, ee, h).start()
                    spread(ee, y, h, k, side)
                    if first and k > 0:
                        for yy in others_of(y):
                            arrived(ee, 2 * yy + c, h)
                            spread(ee, yy, h, k, side)
                guarded(cond, go)
        if k == 0:
            for h in range(y_first):
                for yy in others_of(y):
                    arrived(e, 2 * yy + c, h)
                    spread(e, yy, h, 0, None)

    def y_stage(k):
        for h in range(y_first, len(ag_spans)):
            for side, ee, cond in side_blocks(k):
                def go(ee=ee, h=h):
                    for yy in others_of(y):
                        arrived(ee, 2 * yy + c, h)
                        sib_copy(ee, yy, h).start()
                guarded(cond, go)

    def hidden_stage(k):
        for side, ee, cond in side_blocks(k):
            def go(ee=ee):
                for h in range(len(ag_spans)):
                    for yy in range(Y):
                        arrived(ee, 2 * yy + (1 - c), h)
                mix[...] = jnp.zeros_like(mix)

                @pl.loop(0, D // ktile)
                def _(i):
                    at = pl.ds(pl.multiple_of(i * ktile, ktile), ktile)
                    mix[...] += jnp.dot(tok[ee, :, at], wgu[at, :], preferred_element_type=F32)
                gate, up = mix[:, :U], mix[:, U:]
                hid[ee] = (gate / (1.0 + jnp.exp(-gate)) * up).astype(BF16)
            guarded(cond, go)

    for k in range(E):
        z_stage(k)
        if k == 1:
            loads[0].wait()
        if k >= 1:
            y_stage(k - 1)
            hidden_stage(k - 1)
    y_stage(E - 1)
    hidden_stage(E - 1)
    loads[1].wait()
    for i, j in others:
        src = cw_all.at[(e + E - i) % E, (yc + EY - j) % EY]
        remote(src, src, cw_s.at[i, j], cw_r.at[(e + E - i) % E, (yc + EY - j) % EY], sib).wait_recv()

    high = (2 * e) // E
    order = []
    for j in range(E):
        a = E - 1 - j // 2 if j % 2 == 0 else j // 2
        order.append(a + high * (E - 1 - 2 * a))

    def own(t, yy, span):
        return part.at[t, rows(2 * yy + c), pl.ds(*span)]

    def rsib_copy(t, yy):
        return remote(part.at[t, rows(2 * yy + 1 - c)], sib_in.at[t, yy], rsib_s.at[t, yy], rsib_r.at[t, yy], sib)

    def ry_copy(i, t, h):
        yy = (y + 1 + i) % Y
        return remote(own(t, yy, rs_spans[h]), y_in.at[i, t, :, pl.ds(*rs_spans[h])], ry_s.at[i, t, h],
                      ry_r.at[i, t, h], {"ey": 2 * yy + c})

    def rz_copy(way, t, h):
        return remote(own(t, y, rs_spans[h]), z_in.at[way, t, :, pl.ds(*rs_spans[h])], rz_s.at[way, t, h],
                      rz_r.at[way, t, h], {"ex": e + 1 - 2 * way})

    pick = (lax.broadcasted_iota(jnp.int32, (R, LANES), 0) == lax.broadcasted_iota(jnp.int32, (R, LANES), 1))

    def local_stage(t):
        cols = [jnp.sum(jnp.where(pick, cw_all[t, cc, pl.ds(yc, 1), :], 0.0), axis=1, keepdims=True) for cc in range(EY)]
        scale = jnp.concatenate(cols, axis=0)

        @pl.loop(0, D // ntile)
        def _(i):
            at = pl.ds(pl.multiple_of(i * ntile, ntile), ntile)
            part[t, :, at] = (jnp.dot(hid[t], wd[:, at], preferred_element_type=F32) * scale).astype(BF16)
        for i in range(Y):
            rsib_copy(t, (y + 1 + i) % Y).start()

    def pair_stage(t):
        for i in range(Y - 1):
            yy = (y + 1 + i) % Y
            rsib_copy(t, yy).wait_recv()
            for h, (lo, n) in enumerate(rs_spans):
                cut = pl.ds(lo, n)
                total = part[t, rows(2 * yy + c), cut].astype(F32) + sib_in[t, yy, :, cut].astype(F32)
                part[t, rows(2 * yy + c), cut] = total.astype(BF16)
                ry_copy(i, t, h).start()

    def line_stage(t):
        rsib_copy(t, y).wait_recv()
        for h, (lo, n) in enumerate(rs_spans):
            cut = pl.ds(lo, n)
            for i in range(Y - 1):
                ry_copy(i, t, h).wait_recv()
            total = part[t, rows(yc), cut].astype(F32) + sib_in[t, y, :, cut].astype(F32)
            for i in range(Y - 1):
                total = total + y_in[i, t, :, cut].astype(F32)
            acc[:, pl.ds(0, n)] = total
            for way, onward, behind in ((0, t > e, e > 0), (1, t < e, e < E - 1)):
                @pl.when(onward & behind)
                def _():
                    rz_copy(way, t, h).wait_recv()
                    acc[:, pl.ds(0, n)] += z_in[way, t, :, cut].astype(F32)
            part[t, rows(yc), cut] = acc[:, pl.ds(0, n)].astype(BF16)
            for way, onward in ((0, t > e), (1, t < e)):
                @pl.when(onward)
                def _():
                    rz_copy(way, t, h).start()

    for j in range(E):
        local_stage(order[j])
        pair_stage(order[j])
        if j >= 1:
            line_stage(order[j - 1])
    line_stage(order[E - 1])
    for h, (lo, n) in enumerate(rs_spans):
        cut = pl.ds(lo, n)
        acc[:, pl.ds(0, n)] = part[e, rows(yc), cut].astype(F32) + tok[e, rows(yc), cut].astype(F32)
        for way, behind in ((0, e > 0), (1, e < E - 1)):
            @pl.when(behind)
            def _():
                rz_copy(way, e, h).wait_recv()
                acc[:, pl.ds(0, n)] += z_in[way, e, :, cut].astype(F32)
        out_ref[:, cut] = acc[:, pl.ds(0, n)].astype(BF16)

    for h in range(len(ag_spans)):
        shift_copy(h).wait_send()
    for i, j in others:
        cw_copy(i, j).wait_send()
    for ee in range(E):
        for h in range(len(ag_spans)):
            for yy in range(Y):
                sib_copy(ee, yy, h).wait_send()
            for i in range(Y - 1):
                if h >= y_first:
                    y_copy(i, ee, h).wait_send()
                else:
                    pl.when(e == ee)(lambda i=i, ee=ee, h=h: y_copy(i, ee, h).wait_send())
            for way, going in ((0, (e >= ee) & (e < E - 1)), (1, (e <= ee) & (e > 0))):
                @pl.when(going)
                def _():
                    for yy in ([y] + others_of(y) if h < y_first else [y]):
                        z_copy(way, ee, yy, h).wait_send()
    for t in range(E):
        for yy in range(Y):
            rsib_copy(t, yy).wait_send()
        for h in range(len(rs_spans)):
            for i in range(Y - 1):
                ry_copy(i, t, h).wait_send()
            for way, going in ((0, t > e), (1, t < e)):
                @pl.when(going)
                def _():
                    rz_copy(way, t, h).wait_send()


def fused(section_out, weights, gate_up, down_rows):
    S, E, EY = lax.axis_size("section"), lax.axis_size("ex"), lax.axis_size("ey")
    Y = EY // 2
    R, D = section_out.shape
    U = down_rows.shape[0]
    ag_spans, y_first = spans_of(D, 4), 1
    rs_spans = even_spans(D, 4)
    na, nr = len(ag_spans), len(rs_spans)
    widest = max(n for _, n in rs_spans)
    dma = pltpu.SemaphoreType.DMA
    kernel = functools.partial(fused_kernel, S, E, EY, R, D, U, weights.shape[0], ag_spans, y_first, rs_spans, 512, 512)
    anywhere, vmem = pl.BlockSpec(memory_space=pl.ANY), pl.BlockSpec(memory_space=pltpu.VMEM)
    return pl.pallas_call(
        kernel,
        out_shape=jax.ShapeDtypeStruct((R, D), BF16),
        in_specs=[anywhere, vmem, anywhere, anywhere],
        out_specs=vmem,
        scratch_shapes=[
            pltpu.VMEM((E, EY * R, D), BF16),
            pltpu.VMEM((E, EY * R, D), BF16),
            pltpu.VMEM((D, 2 * U), BF16),
            pltpu.VMEM((U, D), BF16),
            pltpu.VMEM((E, EY * R, U), BF16),
            pltpu.VMEM((EY * R, 2 * U), F32),
            pltpu.VMEM((R, widest), F32),
            pltpu.VMEM((E, EY) + weights.shape, F32),
            pltpu.VMEM((E, Y, R, D), BF16),
            pltpu.VMEM((Y - 1, E, R, D), BF16),
            pltpu.VMEM((2, E, R, D), BF16),
            dma((2,)), dma((na,)), dma((E, EY, na)), dma((2, E, Y, na)), dma((Y - 1, E, na)), dma((E, Y, na)),
            dma((E, EY)), dma((E, EY)),
            dma((E, Y)), dma((E, Y)), dma((Y - 1, E, nr)), dma((Y - 1, E, nr)), dma((2, E, nr)), dma((2, E, nr)),
        ],
        compiler_params=pltpu.CompilerParams(collective_id=0, has_side_effects=True, vmem_limit_bytes=VMEM_BYTES),
    )(section_out, weights, gate_up, down_rows)


def plain(section_out, own_weights, gate_up, down_rows):
    S = lax.axis_size("section")
    U = down_rows.shape[0]
    incoming = lax.ppermute(section_out, "section", [(i, (i + 1) % S) for i in range(S)])
    tokens = lax.all_gather(incoming, ("ex", "ey"), axis=0, tiled=True)
    scale = lax.all_gather(own_weights, ("ex", "ey"), axis=1, tiled=True)
    scale = lax.dynamic_index_in_dim(scale, lax.axis_index("ey"), 0, keepdims=False)
    mixed = jnp.dot(tokens, gate_up, preferred_element_type=F32)
    hidden = (jax.nn.silu(mixed[:, :U]) * mixed[:, U:]).astype(BF16)
    parts = (jnp.dot(hidden, down_rows, preferred_element_type=F32) * scale[:, None]).astype(BF16)
    total = lax.psum_scatter(parts, ("ex", "ey"), scatter_dimension=0, tiled=True)
    return (incoming.astype(F32) + total.astype(F32)).astype(BF16)


def on_device(section_out, expert_ids, gate_weights, w_gate_up, w_down):
    E, EY = lax.axis_size("ex"), lax.axis_size("ey")
    Y = EY // 2
    R, D = section_out.shape[1:]
    U = w_down.shape[2]
    gate_up = w_gate_up[0, 0].reshape(D, 2 * U)
    down_rows = w_down[0, 0]
    named = expert_ids[0][None] == jnp.arange(EY, dtype=jnp.int32)[:, None, None]
    own_weights = jnp.sum(jnp.where(named, gate_weights[0][None], 0.0), axis=2)
    blocks = 2 * E * EY + E * Y + E * (Y - 1) + 2 * E + 2
    needed = 2 * R * D * blocks + 6 * U * D + EY * R * U * (2 * E + 16) + (1 << 21)
    if needed > VMEM_BYTES or R > LANES:
        return plain(section_out[0], own_weights, gate_up, down_rows)[None]
    padded = jnp.pad(own_weights, ((0, -EY % 8), (0, LANES - R)))
    return fused(section_out[0], padded, gate_up, down_rows)[None]


def solution(mesh):
    return jax.shard_map(
        on_device,
        mesh=mesh,
        in_specs=(
            P("section", ("ex", "ey"), None),
            P("section", ("ex", "ey"), None),
            P("section", ("ex", "ey"), None),
            P("section", "ey", None, None, "ex"),
            P("section", "ey", "ex", None),
        ),
        out_specs=P("section", ("ex", "ey"), None),
        check_vma=False,
    )
```

```python
import functools
import jax
import jax.numpy as jnp
from jax import lax
from jax.experimental import pallas as pl
from jax.experimental.pallas import tpu as pltpu
from jax.sharding import PartitionSpec as P

LANES = 128
VMEM_BYTES = 67043328
MESH = pl.DeviceIdType.MESH
SHIFT_AHEAD = 2
LAG = 2
F32, BF16 = jnp.float32, jnp.bfloat16


def spans_of(width, parts):
    tiles = width // LANES
    first = max(1, tiles * 10 // 56)
    cuts = [0, first * LANES]
    for i in range(parts - 1):
        cuts.append((first + (tiles - first) * (i + 1) // (parts - 1)) * LANES)
    return tuple((a, b - a) for a, b in zip(cuts[:-1], cuts[1:]))


def even_spans(width, parts):
    tiles = width // LANES
    cuts = [tiles * i // parts * LANES for i in range(parts + 1)]
    return tuple((a, b - a) for a, b in zip(cuts[:-1], cuts[1:]))


def fused_kernel(S, E, EY, R, D, U, CAPW, ag_spans, y_first, rs_spans, ktile, ntile,
                 x_ref, cw_ref, wgu_ref, wd_ref, out_ref,
                 tok, part, wgu, wd, hid, mix, acc, cw_all, sib_in, y_in, z_in,
                 w_sem, shift_s, ag_r, zs, ys, ss, cw_s, cw_r,
                 rsib_s, rsib_r, ry_s, ry_r, rz_s, rz_r):
    Y = EY // 2
    s, e, yc = lax.axis_index("section"), lax.axis_index("ex"), lax.axis_index("ey")
    y, c = yc // 2, yc % 2
    sib = {"ey": 2 * y + (1 - c)}

    barrier = pltpu.get_barrier_semaphore()
    others = [(i, j) for i in range(E) for j in range(EY) if i or j]
    for i, j in others:
        pl.semaphore_signal(barrier, inc=1, device_id={"ex": (e + i) % E, "ey": (yc + j) % EY}, device_id_type=MESH)
    for d in (1, S - 1):
        pl.semaphore_signal(barrier, inc=1, device_id={"section": (s + d) % S}, device_id_type=MESH)
    loads = [pltpu.make_async_copy(wgu_ref, wgu, w_sem.at[0]), pltpu.make_async_copy(wd_ref, wd, w_sem.at[1])]
    for load in loads:
        load.start()
    pl.semaphore_wait(barrier, len(others) + 2)

    def remote(src, dst, send, recv, device):
        return pltpu.make_async_remote_copy(src_ref=src, dst_ref=dst, send_sem=send, recv_sem=recv,
                                            device_id=device, device_id_type=MESH)

    def rows(core):
        return pl.ds(pl.multiple_of(core * R, R), R)

    def block(ee, cc, h):
        return tok.at[ee, rows(cc), pl.ds(*ag_spans[h])]

    def shift_copy(h):
        return remote(x_ref.at[:, pl.ds(*ag_spans[h])], block(e, yc, h), shift_s.at[h], ag_r.at[e, yc, h],
                      {"section": (s + 1) % S})

    def z_copy(way, ee, yy, h):
        step = 1 - 2 * way
        b = block(ee, 2 * yy + c, h)
        return remote(b, b, zs.at[way, ee, yy, h], ag_r.at[ee, 2 * yy + c, h], {"ex": e + step})

    def y_copy(i, ee, h):
        b = block(ee, yc, h)
        return remote(b, b, ys.at[i, ee, h], ag_r.at[ee, yc, h], {"ey": (yc + 2 * (i + 1)) % EY})

    def sib_copy(ee, yy, h):
        b = block(ee, 2 * yy + c, h)
        return remote(b, b, ss.at[ee, yy, h], ag_r.at[ee, 2 * yy + c, h], sib)

    def arrived(ee, cc, h):
        b = block(ee, cc, h)
        remote(b, b, ss.at[0, 0, 0], ag_r.at[ee, cc, h], sib).wait_recv()

    for h in range(SHIFT_AHEAD):
        shift_copy(h).start()

    def cw_copy(i, j):
        return remote(cw_ref, cw_all.at[e, yc], cw_s.at[i, j], cw_r.at[e, yc],
                      {"ex": (e + i) % E, "ey": (yc + j) % EY})

    for i, j in others:
        cw_copy(i, j).start()
    cw_all[e, yc] = cw_ref[...]

    def spread(ee, yy, h, k, side):
        sib_copy(ee, yy, h).start()
        if side in (None, 0):
            @pl.when(e < E - 1)
            def _():
                z_copy(0, ee, yy, h).start()
        if side in (None, 1):
            @pl.when(e > 0)
            def _():
                z_copy(1, ee, yy, h).start()

    def side_blocks(k):
        if k == 0:
            return [(None, e, None)]
        return [(0, e - k, e >= k), (1, e + k, e + k < E)]

    def guarded(cond, fn):
        if cond is None:
            fn()
        else:
            pl.when(cond)(fn)

    def others_of(y0):
        return [(y0 + 1 + i) % Y for i in range(Y - 1)]

    def z_stage(k):
        for h in range(len(ag_spans)):
            for side, ee, cond in side_blocks(k):
                def go(side=side, ee=ee, h=h):
                    first = h < y_first
                    arrived(ee, yc, h)
                    if k == 0 and h + SHIFT_AHEAD < len(ag_spans):
                        shift_copy(h + SHIFT_AHEAD).start()
                    if not first or k == 0:
                        for i in range(Y - 1):
                            y_copy(i, ee, h).start()
                    spread(ee, y, h, k, side)
                guarded(cond, go)
        for h in range(y_first):
            for side, ee, cond in side_blocks(k):
                def go(side=side, ee=ee, h=h):
                    for yy in others_of(y):
                        arrived(ee, 2 * yy + c, h)
                        spread(ee, yy, h, k, side)
                guarded(cond, go)

    def y_stage(k):
        for h in range(y_first, len(ag_spans)):
            for side, ee, cond in side_blocks(k):
                def go(ee=ee, h=h):
                    for yy in others_of(y):
                        arrived(ee, 2 * yy + c, h)
                        sib_copy(ee, yy, h).start()
                guarded(cond, go)

    def hidden_stage(k):
        for side, ee, cond in side_blocks(k):
            def go(ee=ee):
                for h in range(len(ag_spans)):
                    for yy in range(Y):
                        arrived(ee, 2 * yy + (1 - c), h)
                mix[...] = jnp.zeros_like(mix)

                @pl.loop(0, D // ktile)
                def _(i):
                    at = pl.ds(pl.multiple_of(i * ktile, ktile), ktile)
                    mix[...] += jnp.dot(tok[ee, :, at], wgu[at, :], preferred_element_type=F32)
                gate, up = mix[:, :U], mix[:, U:]
                hid[ee] = (gate / (1.0 + jnp.exp(-gate)) * up).astype(BF16)
            guarded(cond, go)

    for k in range(E):
        z_stage(k)
        if k == 1:
            loads[0].wait()
        if k >= 1:
            y_stage(k - 1)
            hidden_stage(k - 1)
    y_stage(E - 1)
    hidden_stage(E - 1)
    loads[1].wait()
    for i, j in others:
        src = cw_all.at[(e + E - i) % E, (yc + EY - j) % EY]
        remote(src, src, cw_s.at[i, j], cw_r.at[(e + E - i) % E, (yc + EY - j) % EY], sib).wait_recv()

    high = (2 * e) // E
    order = []
    for j in range(E):
        a = E - 1 - j // 2 if j % 2 == 0 else j // 2
        order.append(a + high * (E - 1 - 2 * a))

    def own(t, yy, span):
        return part.at[t, rows(2 * yy + c), pl.ds(*span)]

    def rsib_copy(t, yy):
        return remote(part.at[t, rows(2 * yy + 1 - c)], sib_in.at[t, yy], rsib_s.at[t, yy], rsib_r.at[t, yy], sib)

    def ry_copy(i, t, h):
        yy = (y + 1 + i) % Y
        return remote(own(t, yy, rs_spans[h]), y_in.at[i, t, :, pl.ds(*rs_spans[h])], ry_s.at[i, t, h],
                      ry_r.at[i, t, h], {"ey": 2 * yy + c})

    def rz_copy(way, t, h):
        return remote(own(t, y, rs_spans[h]), z_in.at[way, t, :, pl.ds(*rs_spans[h])], rz_s.at[way, t, h],
                      rz_r.at[way, t, h], {"ex": e + 1 - 2 * way})

    pick = (lax.broadcasted_iota(jnp.int32, (R, LANES), 0) == lax.broadcasted_iota(jnp.int32, (R, LANES), 1))

    def local_stage(t):
        cols = [jnp.sum(jnp.where(pick, cw_all[t, cc, pl.ds(yc, 1), :], 0.0), axis=1, keepdims=True) for cc in range(EY)]
        scale = jnp.concatenate(cols, axis=0)

        @pl.loop(0, D // ntile)
        def _(i):
            at = pl.ds(pl.multiple_of(i * ntile, ntile), ntile)
            part[t, :, at] = (jnp.dot(hid[t], wd[:, at], preferred_element_type=F32) * scale).astype(BF16)
        for i in range(Y):
            rsib_copy(t, (y + 1 + i) % Y).start()

    def pair_stage(t, h):
        cut = pl.ds(*rs_spans[h])
        for i in range(Y - 1):
            yy = (y + 1 + i) % Y
            if h == 0:
                rsib_copy(t, yy).wait_recv()
            total = part[t, rows(2 * yy + c), cut].astype(F32) + sib_in[t, yy, :, cut].astype(F32)
            part[t, rows(2 * yy + c), cut] = total.astype(BF16)
            ry_copy(i, t, h).start()

    def line_stage(t, h):
        lo, n = rs_spans[h]
        cut = pl.ds(lo, n)
        if h == 0:
            rsib_copy(t, y).wait_recv()
        for i in range(Y - 1):
            ry_copy(i, t, h).wait_recv()
        total = part[t, rows(yc), cut].astype(F32) + sib_in[t, y, :, cut].astype(F32)
        for i in range(Y - 1):
            total = total + y_in[i, t, :, cut].astype(F32)
        acc[:, pl.ds(0, n)] = total
        for way, onward, behind in ((0, t > e, e > 0), (1, t < e, e < E - 1)):
            @pl.when(onward & behind)
            def _():
                rz_copy(way, t, h).wait_recv()
                acc[:, pl.ds(0, n)] += z_in[way, t, :, cut].astype(F32)
        part[t, rows(yc), cut] = acc[:, pl.ds(0, n)].astype(BF16)
        for way, onward in ((0, t > e), (1, t < e)):
            @pl.when(onward)
            def _():
                rz_copy(way, t, h).start()

    spans = len(rs_spans)
    local_stage(order[0])
    for g in range(E * spans + LAG):
        if g < E * spans:
            pair_stage(order[g // spans], g % spans)
            if g % spans == 1 and g // spans + 1 < E:
                local_stage(order[g // spans + 1])
        if g >= LAG:
            line_stage(order[(g - LAG) // spans], (g - LAG) % spans)
    for h, (lo, n) in enumerate(rs_spans):
        cut = pl.ds(lo, n)
        acc[:, pl.ds(0, n)] = part[e, rows(yc), cut].astype(F32) + tok[e, rows(yc), cut].astype(F32)
        for way, behind in ((0, e > 0), (1, e < E - 1)):
            @pl.when(behind)
            def _():
                rz_copy(way, e, h).wait_recv()
                acc[:, pl.ds(0, n)] += z_in[way, e, :, cut].astype(F32)
        out_ref[:, cut] = acc[:, pl.ds(0, n)].astype(BF16)

    for h in range(len(ag_spans)):
        shift_copy(h).wait_send()
    for i, j in others:
        cw_copy(i, j).wait_send()
    for ee in range(E):
        for h in range(len(ag_spans)):
            for yy in range(Y):
                sib_copy(ee, yy, h).wait_send()
            for i in range(Y - 1):
                if h >= y_first:
                    y_copy(i, ee, h).wait_send()
                else:
                    pl.when(e == ee)(lambda i=i, ee=ee, h=h: y_copy(i, ee, h).wait_send())
            for way, going in ((0, (e >= ee) & (e < E - 1)), (1, (e <= ee) & (e > 0))):
                @pl.when(going)
                def _():
                    for yy in ([y] + others_of(y) if h < y_first else [y]):
                        z_copy(way, ee, yy, h).wait_send()
    for t in range(E):
        for yy in range(Y):
            rsib_copy(t, yy).wait_send()
        for h in range(len(rs_spans)):
            for i in range(Y - 1):
                ry_copy(i, t, h).wait_send()
            for way, going in ((0, t > e), (1, t < e)):
                @pl.when(going)
                def _():
                    rz_copy(way, t, h).wait_send()


def fused(section_out, weights, gate_up, down_rows):
    S, E, EY = lax.axis_size("section"), lax.axis_size("ex"), lax.axis_size("ey")
    Y = EY // 2
    R, D = section_out.shape
    U = down_rows.shape[0]
    ag_spans, y_first = spans_of(D, 7), 1
    rs_spans = even_spans(D, 7)
    na, nr = len(ag_spans), len(rs_spans)
    widest = max(n for _, n in rs_spans)
    dma = pltpu.SemaphoreType.DMA
    kernel = functools.partial(fused_kernel, S, E, EY, R, D, U, weights.shape[0], ag_spans, y_first, rs_spans, 512, 512)
    anywhere, vmem = pl.BlockSpec(memory_space=pl.ANY), pl.BlockSpec(memory_space=pltpu.VMEM)
    return pl.pallas_call(
        kernel,
        out_shape=jax.ShapeDtypeStruct((R, D), BF16),
        in_specs=[anywhere, vmem, anywhere, anywhere],
        out_specs=vmem,
        scratch_shapes=[
            pltpu.VMEM((E, EY * R, D), BF16),
            pltpu.VMEM((E, EY * R, D), BF16),
            pltpu.VMEM((D, 2 * U), BF16),
            pltpu.VMEM((U, D), BF16),
            pltpu.VMEM((E, EY * R, U), BF16),
            pltpu.VMEM((EY * R, 2 * U), F32),
            pltpu.VMEM((R, widest), F32),
            pltpu.VMEM((E, EY) + weights.shape, F32),
            pltpu.VMEM((E, Y, R, D), BF16),
            pltpu.VMEM((Y - 1, E, R, D), BF16),
            pltpu.VMEM((2, E, R, D), BF16),
            dma((2,)), dma((na,)), dma((E, EY, na)), dma((2, E, Y, na)), dma((Y - 1, E, na)), dma((E, Y, na)),
            dma((E, EY)), dma((E, EY)),
            dma((E, Y)), dma((E, Y)), dma((Y - 1, E, nr)), dma((Y - 1, E, nr)), dma((2, E, nr)), dma((2, E, nr)),
        ],
        compiler_params=pltpu.CompilerParams(collective_id=0, has_side_effects=True, vmem_limit_bytes=VMEM_BYTES),
    )(section_out, weights, gate_up, down_rows)


def plain(section_out, own_weights, gate_up, down_rows):
    S = lax.axis_size("section")
    U = down_rows.shape[0]
    incoming = lax.ppermute(section_out, "section", [(i, (i + 1) % S) for i in range(S)])
    tokens = lax.all_gather(incoming, ("ex", "ey"), axis=0, tiled=True)
    scale = lax.all_gather(own_weights, ("ex", "ey"), axis=1, tiled=True)
    scale = lax.dynamic_index_in_dim(scale, lax.axis_index("ey"), 0, keepdims=False)
    mixed = jnp.dot(tokens, gate_up, preferred_element_type=F32)
    hidden = (jax.nn.silu(mixed[:, :U]) * mixed[:, U:]).astype(BF16)
    parts = (jnp.dot(hidden, down_rows, preferred_element_type=F32) * scale[:, None]).astype(BF16)
    total = lax.psum_scatter(parts, ("ex", "ey"), scatter_dimension=0, tiled=True)
    return (incoming.astype(F32) + total.astype(F32)).astype(BF16)


def on_device(section_out, expert_ids, gate_weights, w_gate_up, w_down):
    E, EY = lax.axis_size("ex"), lax.axis_size("ey")
    Y = EY // 2
    R, D = section_out.shape[1:]
    U = w_down.shape[2]
    gate_up = w_gate_up[0, 0].reshape(D, 2 * U)
    down_rows = w_down[0, 0]
    named = expert_ids[0][None] == jnp.arange(EY, dtype=jnp.int32)[:, None, None]
    own_weights = jnp.sum(jnp.where(named, gate_weights[0][None], 0.0), axis=2)
    blocks = 2 * E * EY + E * Y + E * (Y - 1) + 2 * E + 2
    needed = 2 * R * D * blocks + 6 * U * D + EY * R * U * (2 * E + 16) + (1 << 21)
    if needed > VMEM_BYTES or R > LANES:
        return plain(section_out[0], own_weights, gate_up, down_rows)[None]
    padded = jnp.pad(own_weights, ((0, -EY % 8), (0, LANES - R)))
    return fused(section_out[0], padded, gate_up, down_rows)[None]


def solution(mesh):
    return jax.shard_map(
        on_device,
        mesh=mesh,
        in_specs=(
            P("section", ("ex", "ey"), None),
            P("section", ("ex", "ey"), None),
            P("section", ("ex", "ey"), None),
            P("section", "ey", None, None, "ex"),
            P("section", "ey", "ex", None),
        ),
        out_specs=P("section", ("ex", "ey"), None),
        check_vma=False,
    )
```
